32 devices in a mesh: parts: 2 (over y), pair: 4 (over x, core), sub: 4 (over z).
Axes of the slice: x: 2, y: 2, z: 4, core: 2. Of those that a mesh axis runs over, the one named last changes fastest.
Arguments:
- features: bfloat16 [64, 1024, 256], P(('parts', 'pair'), 'sub'), parts along dimension 0, may hold values from -7 to 7
- counts: int32 [64], P('parts'), parts along dimension 0, may hold values from 256 to 1024
- pair_table: int32 [8, 4, 2], P('parts'), parts along dimension 0, may hold values from -1 to 31, as said below
- w_qk: bfloat16 [256, 256], replicated, may hold values from -0.75 to 0.75
- w_value: bfloat16 [256, 256], replicated, may hold values from -0.375 to 0.375
- w_out: bfloat16 [256, 256], replicated, may hold values from -1.5 to 1.5
- w_merge_in: bfloat16 [512, 512], replicated, may hold values from -0.25 to 0.25
- w_merge_out: bfloat16 [512, 256], replicated, may hold values from -0.25 to 0.25
Outputs:
- updated: bfloat16 [64, 1024, 256], P(('parts', 'pair'), 'sub'), parts along dimension 0
The draws below stay inside these ranges and needn't reach their ends.
There are 2 independent parts, one for each index of `parts`. The reference program is written for one: setup_inputs(seed, part) draws one part's arguments, and reference() takes and returns one part's arrays. A program takes and returns all parts, laid end to end along the dimension named above; an argument that names none is the same for every part. Nothing has to cross between parts.
Inputs may be any that keep to these rules, and one draw needn't show every extreme that they name: `pair_table`: row g lists the pairs owned by index g of pair, one slot per index of sub; -1 in both entries marks an empty slot. A live slot names two images of different groups, image i belonging to group i // 8. Over the live slots of one owner, at most 2 named images (counted with repetition) belong to any one group; some owner has all 4 slots live and reaches that bound for every group.
All inputs are finite; a program needn't handle non-finite values.
Results may differ from the reference program's by a relative error of at most 0.0067.
Values may be sent and summed in bfloat16 or wider, within the bound.
No kernel may reach another device: no remote copies, remote signals or barrier semaphores. Data moves between devices by JAX's collectives and lax.ppermute only.
A program may use at most 64 MiB of HBM per device.

```python
import jax
import jax.numpy as jnp
from jax import lax

D = 256
HEADS = 4
KP = 1024
IMG_GRP = 8
GROUPS = 4
SLOTS = 4
IMAGES = 32
MERGE = 512


def pair_layout(key):
    base_load = 5 * SLOTS // 8
    group_order = jax.random.permutation(jax.random.fold_in(key, 101), GROUPS)
    extra_load = jax.random.randint(jax.random.fold_in(key, 102), (GROUPS // 2,), 0, SLOTS - base_load + 1)
    extra_load = extra_load.at[0].set(SLOTS - base_load)
    group_load = jnp.zeros((GROUPS,), jnp.int32)
    group_load = group_load.at[group_order[0::2]].set(base_load + extra_load)
    group_load = group_load.at[group_order[1::2]].set(base_load - extra_load)
    source_perm = jax.vmap(lambda sub_key: jax.random.permutation(sub_key, GROUPS))(jax.random.split(jax.random.fold_in(key, 103), GROUPS))
    position_src = jnp.take(source_perm, jnp.arange(2 * SLOTS) % GROUPS, axis=1)
    local_index = jax.random.randint(jax.random.fold_in(key, 104), (GROUPS, 2 * SLOTS), 0, IMG_GRP)
    image_id = (position_src * IMG_GRP + local_index).reshape(GROUPS, SLOTS, 2)
    slot_live = jnp.arange(SLOTS)[None, :] < group_load[:, None]
    image_id = jnp.where(slot_live[:, :, None], image_id, -1)
    slot_perm = jax.vmap(lambda sub_key: jax.random.permutation(sub_key, SLOTS))(jax.random.split(jax.random.fold_in(key, 105), GROUPS))
    slot_perm = jnp.repeat(slot_perm[:, :, None], 2, axis=2)
    image_id = jnp.take_along_axis(image_id, slot_perm, axis=1)
    return image_id.astype(jnp.int32)


def draw_pair_table(key, part):
    return pair_layout(key)


def draw_features(key, part):
    shape = (IMAGES, KP, D)
    base_vals = jnp.clip(jax.random.normal(jax.random.fold_in(key, 1), shape, jnp.float32), -4.0, 4.0)
    return base_vals.astype(jnp.bfloat16)


def set_ends(array, key, least, largest):
    extent = array.shape
    place = [jax.random.randint(jax.random.fold_in(key, axis), (), 0, extent[axis]) for axis in range(len(extent))]
    array = array.at[tuple(place)].set(least)
    longest = extent.index(max(extent))
    place[longest] = (place[longest] + 1) % extent[longest]
    return array.at[tuple(place)].set(largest)


def normal_values(key, dims, spread, bound, held_as=jnp.bfloat16):
    return jnp.clip(spread * jax.random.normal(key, dims, jnp.float32), -bound, bound).astype(held_as)


def setup_inputs(seed: int = 0, part: int = 0) -> dict:
    streams_of = jax.random.split(jax.random.key(seed), 9)
    part_keys = jax.random.split(jax.random.fold_in(streams_of[8], part), 9)
    return {
        "features": draw_features(jax.random.fold_in(jax.random.fold_in(streams_of[8], part), 71), part),
        "counts": set_ends(jax.random.randint(part_keys[1], (IMAGES,), KP // 4, KP + 1), jax.random.fold_in(part_keys[1], 1), KP // 4, KP).astype(jnp.int32),
        "pair_table": draw_pair_table(jax.random.fold_in(jax.random.fold_in(streams_of[8], part), 71), part),
        "w_qk": normal_values(streams_of[3], (D, D), (D // 4) ** -0.5, 0.75),
        "w_value": normal_values(streams_of[4], (D, D), D ** -0.5, 0.375),
        "w_out": normal_values(streams_of[5], (D, D), (D // 16) ** -0.5, 1.5),
        "w_merge_in": normal_values(streams_of[6], (MERGE, MERGE), MERGE ** -0.5, 0.25),
        "w_merge_out": normal_values(streams_of[7], (MERGE, D), MERGE ** -0.5, 0.25),
    }


ln_eps = 1e-05

def layer_norm(hidden):
    center = lax.optimization_barrier(jnp.mean(hidden, axis=-1, keepdims=True))
    centered = hidden - center
    variance = lax.optimization_barrier(jnp.mean(centered * centered, axis=-1, keepdims=True))
    return centered * lax.rsqrt(variance + ln_eps)

def pair_messages(left_feats, right_feats, left_count, right_count, w_qk, w_value, head_count):
    points = left_feats.shape[0]
    model_width = left_feats.shape[1]
    head_dim = model_width // head_count
    stacked = jnp.concatenate([left_feats, right_feats], axis=0)
    query_key = jnp.dot(stacked, w_qk, preferred_element_type=jnp.float32).astype(jnp.bfloat16)
    values = jnp.dot(stacked, w_value, preferred_element_type=jnp.float32).astype(jnp.bfloat16)
    row_ids = lax.broadcasted_iota(jnp.int32, (points, 1), 0)
    col_ids = lax.broadcasted_iota(jnp.int32, (1, points), 1)
    col_valid = col_ids < right_count
    row_valid = row_ids < left_count
    score_scale = head_dim ** (-0.5)
    to_left = []
    to_right = []
    for head_index in range(head_count):
        head_lo = head_index * head_dim
        q_left = query_key[:points, head_lo:head_lo + head_dim]
        q_right = query_key[points:, head_lo:head_lo + head_dim]
        v_left = values[:points, head_lo:head_lo + head_dim]
        v_right = values[points:, head_lo:head_lo + head_dim]
        scores = lax.dot_general(q_left, q_right, (((1,), (1,)), ((), ())), preferred_element_type=jnp.float32) * score_scale
        masked = jnp.where(col_valid, scores, -jnp.inf)
        row_top = lax.optimization_barrier(jnp.max(masked, axis=1, keepdims=True))
        row_exp = jnp.exp(masked - row_top)
        row_total = lax.optimization_barrier(jnp.sum(row_exp, axis=1, keepdims=True))
        to_left.append(jnp.dot(row_exp.astype(jnp.bfloat16), v_right, preferred_element_type=jnp.float32) / row_total)
        col_masked = jnp.where(row_valid, scores, -jnp.inf)
        col_top = lax.optimization_barrier(jnp.max(col_masked, axis=0, keepdims=True))
        col_exp = jnp.exp(col_masked - col_top)
        col_total = lax.optimization_barrier(jnp.sum(col_exp, axis=0, keepdims=True))
        summed = lax.dot_general(col_exp.astype(jnp.bfloat16), v_left, (((0,), (0,)), ((), ())), preferred_element_type=jnp.float32)
        to_right.append(summed / col_total.reshape(points, 1))
    return (jnp.concatenate(to_left, axis=1).astype(jnp.bfloat16), jnp.concatenate(to_right, axis=1).astype(jnp.bfloat16))

def reference(features, counts, pair_table, w_qk, w_value, w_out, w_merge_in, w_merge_out):
    images, points, model_width = features.shape
    slot_list = pair_table.reshape(-1, 2).astype(jnp.int32)

    def add_slot(msg_total, slot):
        left_id = jnp.maximum(slot[0], 0).astype(jnp.int32)
        right_id = jnp.maximum(slot[1], 0).astype(jnp.int32)

        def work(carried):
            left_feats = lax.dynamic_index_in_dim(features, left_id, 0, keepdims=False)
            right_feats = lax.dynamic_index_in_dim(features, right_id, 0, keepdims=False)
            left_count = lax.dynamic_index_in_dim(counts, left_id, 0, keepdims=False)
            right_count = lax.dynamic_index_in_dim(counts, right_id, 0, keepdims=False)
            to_left, to_right = pair_messages(left_feats, right_feats, left_count, right_count, w_qk, w_value, HEADS)
            carried = carried.at[left_id].add(to_left.astype(jnp.float32))
            carried = carried.at[right_id].add(to_right.astype(jnp.float32))
            return carried
        msg_total = lax.cond(slot[0] >= 0, work, lambda carried: carried, msg_total)
        return (msg_total, None)
    msg_total, _ = lax.scan(add_slot, jnp.zeros((images, points, model_width), jnp.float32), slot_list)
    image_ids = jnp.arange(images).astype(jnp.int32)
    use_count = lax.optimization_barrier(jnp.sum((slot_list.reshape(1, -1) == image_ids[:, None]).astype(jnp.int32), axis=1))
    divisor = jnp.maximum(use_count, 1).astype(jnp.float32)
    mean_msg = (msg_total / divisor[:, None, None]).astype(jnp.bfloat16)
    own_rows = features.reshape(-1, model_width)
    lifted = jnp.dot(mean_msg.reshape(-1, model_width), w_out, preferred_element_type=jnp.float32).astype(jnp.bfloat16)
    hidden = jnp.dot(own_rows, w_merge_in[:model_width], preferred_element_type=jnp.float32)
    hidden = hidden + jnp.dot(lifted, w_merge_in[model_width:], preferred_element_type=jnp.float32)
    active = jax.nn.gelu(layer_norm(hidden), approximate=False).astype(jnp.bfloat16)
    updated = own_rows.astype(jnp.float32) + jnp.dot(active, w_merge_out, preferred_element_type=jnp.float32)
    return updated.astype(jnp.bfloat16).reshape(images, points, model_width)
```

```python
import functools

import jax
import jax.numpy as jnp
from jax import lax
from jax.experimental import pallas as pl
from jax.experimental.pallas import tpu as pltpu
from jax.sharding import PartitionSpec as P

HEADS = 4
CHUNKS = 2
LN_EPS = 1e-05
SUM_LOW = 1e-25
SUM_HIGH = 1e25


F32 = jnp.float32
BF16 = jnp.bfloat16
SMEM = pltpu.SMEM
VMEM = pltpu.VMEM


def dot(a, b, dims=(((1,), (0,)), ((), ()))):
    return lax.dot_general(a, b, dims, preferred_element_type=F32)


class Layout:
    def __init__(self, n_pair, n_sub, img_grp):
        self.n_pair, self.n_sub, self.img_grp = n_pair, n_sub, img_grp
        self.per_src = 2 * n_sub // n_pair
        self.n_msg = n_pair * self.per_src
        at = 0
        for name, size in (
            ("send", self.n_msg),
            ("zsel", 2 * n_sub),
            ("xret", self.n_msg),
            ("live", 1),
            ("count", 2),
            ("n_used", 1),
            ("n_idle", 1),
            ("used", img_grp),
            ("idle", img_grp),
            ("uses", img_grp),
            ("mine", img_grp * self.n_msg),
            ("me_sub", 1),
        ):
            setattr(self, name, at)
            at += size
        self.size = at
        few = min(self.per_src, n_sub)
        low = (n_sub - few) // 2
        self.few_low, self.few = low, few
        self.few_hosts = tuple(range(low, low + few))
        self.all_hosts = tuple(range(n_sub))


def table_kernel(lay, ids, table, counts, feats, *refs):
    n_pair, n_sub, per_src = lay.n_pair, lay.n_sub, lay.per_src
    outs, (compact_ref, tab), (host, used_up) = refs[:-4], refs[-4:-2], refs[-2:]
    slots = n_pair * n_sub
    me_g, me_s = ids[0], ids[1]

    def clear(i, c):
        tab[i] = 0
        return c

    lax.fori_loop(0, lay.size, clear, 0)
    for i in range(n_pair * n_pair):
        used_up[i] = 0
    total = lax.fori_loop(
        0, slots, lambda k, c: c + (table[2 * k] >= 0).astype(jnp.int32), jnp.int32(0)
    )
    compact = total <= n_pair * lay.few
    compact_ref[0] = compact.astype(jnp.int32)

    @pl.when(compact)
    def _():
        def wipe(k, c):
            host[k] = -1
            return c

        lax.fori_loop(0, 2 * slots, wipe, 0)

        def place(k, rank):
            live = table[2 * k] >= 0

            @pl.when(live)
            def _():
                at = (rank % n_pair) * n_sub + lay.few_low + rank // n_pair
                host[2 * at] = table[2 * k]
                host[2 * at + 1] = table[2 * k + 1]

            return rank + live.astype(jnp.int32)

        lax.fori_loop(0, slots, place, jnp.int32(0))

    @pl.when(jnp.logical_not(compact))
    def _():
        def same(k, c):
            host[k] = table[k]
            return c

        lax.fori_loop(0, 2 * slots, same, 0)

    def mention(m, c):
        image = host[m]

        @pl.when(image >= 0)
        def _():
            g = m // (2 * n_sub)
            t = (m // 2) % n_sub
            side = m % 2
            p = image // lay.img_grp
            k = used_up[p * n_pair + g]
            used_up[p * n_pair + g] = k + 1

            @pl.when(p == me_g)
            def _():
                entry = (g ^ me_g) * per_src + k
                own = image - p * lay.img_grp
                tab[lay.send + entry] = own
                n = tab[lay.uses + own]
                tab[lay.mine + own * lay.n_msg + n] = entry
                tab[lay.uses + own] = n + 1

            @pl.when(g == me_g)
            def _():
                entry = (p ^ me_g) * per_src + k
                tab[lay.zsel + 2 * t + side] = entry
                tab[lay.xret + entry] = 2 * ((me_s - t + n_sub) % n_sub) + side

                @pl.when(t == me_s)
                def _():
                    tab[lay.live] = 1
                    tab[lay.count + side] = counts[image]

        return c

    lax.fori_loop(0, 2 * slots, mention, 0)
    tab[lay.me_sub] = me_s

    def sort(n, c):
        named = tab[lay.uses + n] > 0

        @pl.when(named)
        def _():
            at = tab[lay.n_used]
            tab[lay.used + at] = n
            tab[lay.n_used] = at + 1

        @pl.when(jnp.logical_not(named))
        def _():
            at = tab[lay.n_idle]
            tab[lay.idle + at] = n
            tab[lay.n_idle] = at + 1

        return c

    lax.fori_loop(0, lay.img_grp, sort, 0)

    rows = feats.shape[1] // CHUNKS
    for r in range(n_pair):
        for k in range(per_src):
            image = tab[lay.send + r * per_src + k]
            for c in range(CHUNKS):
                outs[r * CHUNKS + c][k] = feats[image, c * rows : (c + 1) * rows]


def pick(refs, entry, width, put):
    which, at = entry // width, entry % width
    for r, ref in enumerate(refs):

        @pl.when(which == r)
        def _(ref=ref):
            put(ref[at])


def zpack_kernel(lay, tab, *refs):
    n_sub = lay.n_sub
    arrived, outs = refs[: lay.n_pair], refs[lay.n_pair :]
    for r in range(n_sub):
        t = (tab[lay.me_sub] - r + n_sub) % n_sub
        for side in range(2):

            def put(block, r=r, side=side):
                outs[r][side] = block

            pick(arrived, tab[lay.zsel + 2 * t + side], lay.per_src, put)


def xpack_kernel(lay, tab, *refs):
    returned, outs = refs[: lay.n_sub], refs[lay.n_sub :]
    for r in range(lay.n_pair):
        for k in range(lay.per_src):

            def put(block, r=r, k=k):
                outs[r][k] = block

            pick(returned, tab[lay.xret + r * lay.per_src + k], 2, put)


def attention_kernel(lay, head_dim, tab, w_qk, w_val, w_val_t, *refs):
    n_sub = lay.n_sub
    n_in = n_sub * CHUNKS
    xs, outs = refs[:n_in], refs[n_in:-6]
    x, qk, v_ext, va_t, exps, flag = refs[-6:]
    chunk = xs[0].shape[1]
    kp_block = chunk * CHUNKS
    points = n_sub * kp_block
    width = w_qk.shape[1]
    scale = head_dim ** (-0.5)
    ext = 2 * head_dim
    pairs = HEADS // 2
    half = points // 4

    @pl.when(tab[lay.live] == 1)
    def _():
        for r in range(n_sub):
            for c in range(CHUNKS):
                at = r * kp_block + c * chunk
                for side in range(2):
                    x[side, at : at + chunk] = xs[r * CHUNKS + c][side]

        def valid(shape, axis, side):
            ids = lax.broadcasted_iota(jnp.int32, shape, axis)
            block = ids // kp_block
            pos = ((tab[lay.me_sub] + block) % n_sub) * kp_block + (ids - block * kp_block)
            return pos < tab[lay.count + side]

        lane = lax.broadcasted_iota(jnp.int32, (1, width), 1) // head_dim
        ext_lane = lax.broadcasted_iota(jnp.int32, (1, HEADS * ext), 1)
        is_one = ((ext_lane // head_dim) % 2) != ((ext_lane // ext) % 2)
        ext_row = lax.broadcasted_iota(jnp.int32, (HEADS * ext, 1), 0)
        is_one_t = ((ext_row // head_dim) % 2) == 1

        def project_values(side):
            v = dot(x[side], w_val[...])
            v = jnp.where(is_one, 1.0, v)
            v_ext[...] = jnp.where(valid((points, 1), 0, side), v, 0.0).astype(BF16)

        qk[0] = dot(x[0], w_qk[...]).astype(BF16)
        qk[1] = dot(x[1], w_qk[...]).astype(BF16)
        project_values(1)
        vt = dot(w_val_t[...], x[0], (((1,), (1,)), ((), ())))
        vt = jnp.where(is_one_t, 1.0, vt)
        va_t[...] = jnp.where(valid((1, points), 1, 0), vt, 0.0).astype(BF16)

        def write(side, pair, row, msg):
            for i in range(msg.shape[0] // kp_block):
                at = row // kp_block + i
                part = msg[i * kp_block : (i + 1) * kp_block].astype(BF16)
                outs[at][side, :, pair * ext : (pair + 1) * ext] = part

        low_lane = lax.broadcasted_iota(jnp.int32, (1, ext), 1) < head_dim

        def merge(even, odd):
            top = jnp.where(low_lane, even, odd)
            total = pltpu.roll(jnp.where(low_lane, odd, even), head_dim, 1)
            return top / total, total

        low, high = [], []

        def seen(total):
            low.append(jnp.min(total, keepdims=True))
            high.append(jnp.max(total, keepdims=True))

        for pair in range(pairs):
            sums = []
            for j in range(2):
                h = 2 * pair + j
                sums.append([])
                for i in range(4):
                    q = qk[0, i * half : (i + 1) * half]
                    q = jnp.where(lane == h, q * scale, 0.0).astype(BF16)
                    s = dot(q, qk[1], (((1,), (1,)), ((), ())))
                    e = jnp.exp(s).astype(BF16)
                    exps[j, i * half : (i + 1) * half] = e
                    sums[j].append(dot(e, v_ext[:, h * ext : (h + 1) * ext]))
            for i in range(4):
                msg, total = merge(sums[0][i], sums[1][i])
                seen(total)
                write(0, pair, i * half, msg)
            columns = []
            for j in range(2):
                h = 2 * pair + j
                out = dot(va_t[h * ext : (h + 1) * ext], exps[j])
                total = out[head_dim : head_dim + 1]
                seen(total)
                columns.append(out[:head_dim] / total)
            write(1, pair, 0, jnp.concatenate(columns, axis=0).T)
        smallest = functools.reduce(jnp.minimum, low)
        largest = functools.reduce(jnp.maximum, high)
        sound = (smallest > SUM_LOW) & (largest < SUM_HIGH)
        flag[0] = jnp.max(jnp.where(sound, 1, 0))

        @pl.when(flag[0] == 0)
        def _():
            for side in range(2):
                project_values(1 - side)
                key_ok = valid((1, points), 1, 1 - side)
                for i in range(n_sub):
                    for pair in range(pairs):
                        sums = []
                        for j in range(2):
                            h = 2 * pair + j
                            q = qk[side, i * kp_block : (i + 1) * kp_block]
                            q = jnp.where(lane == h, q * scale, 0.0).astype(BF16)
                            s = dot(q, qk[1 - side], (((1,), (1,)), ((), ())))
                            s = jnp.where(key_ok, s, -jnp.inf)
                            e = jnp.exp(s - jnp.max(s, axis=1, keepdims=True)).astype(BF16)
                            sums.append(dot(e, v_ext[:, h * ext : (h + 1) * ext]))
                        write(side, pair, i * kp_block, merge(*sums)[0])


def update_kernel(lay, with_messages, tab, feats, w_out, w_in, w_up, *refs):
    msgs = refs[: lay.n_pair] if with_messages else ()
    out, total = refs[-2:]
    width = feats.shape[2]

    def step(i, c):
        n = tab[(lay.used if with_messages else lay.idle) + i]
        own = feats[n]
        hidden = dot(own, w_in[:width])
        if with_messages:
            uses = tab[lay.uses + n]
            total[...] = jnp.zeros_like(total)

            def add(k, c):
                def put(block):
                    total[...] += block.astype(F32)

                pick(msgs, tab[lay.mine + n * lay.n_msg + k], lay.per_src, put)
                return c

            lax.fori_loop(0, uses, add, 0)
            mean = (total[...] / uses.astype(F32)).astype(BF16)
            lifted = dot(mean, w_out[...]).astype(BF16)
            hidden = hidden + dot(lifted, w_in[width:])
        centered = hidden - jnp.mean(hidden, axis=-1, keepdims=True)
        variance = jnp.mean(centered * centered, axis=-1, keepdims=True)
        normed = centered * lax.rsqrt(variance + LN_EPS)
        active = 0.5 * normed * (1.0 + lax.erf(normed * (0.5**0.5)))
        new = own.astype(F32) + dot(active.astype(BF16), w_up[...])
        out[n] = new.astype(BF16)
        return c

    lax.fori_loop(0, tab[lay.n_used if with_messages else lay.n_idle], step, 0)


def local(features, counts, pair_table, w_qk, w_value, w_out, w_merge_in, w_merge_out):
    n_pair = lax.axis_size("pair")
    n_sub = lax.axis_size("sub")
    me_g = lax.axis_index("pair")
    me_s = lax.axis_index("sub")
    img_grp, kp_block, width = features.shape
    head_dim = width // HEADS
    lay = Layout(n_pair, n_sub, img_grp)
    per_src = lay.per_src
    rows = kp_block // CHUNKS
    slots = n_pair * n_sub
    smem = pl.BlockSpec(memory_space=SMEM)
    vmem = pl.BlockSpec(memory_space=VMEM)

    def shaped(*dims, dtype=BF16):
        return jax.ShapeDtypeStruct(dims, dtype)

    *sends, compact, tab = pl.pallas_call(
        functools.partial(table_kernel, lay),
        in_specs=[smem, smem, smem, vmem],
        out_specs=[vmem] * (n_pair * CHUNKS) + [smem, smem],
        out_shape=[shaped(per_src, rows, width)] * (n_pair * CHUNKS)
        + [shaped(1, dtype=jnp.int32), shaped(lay.size, dtype=jnp.int32)],
        scratch_shapes=[SMEM((2 * slots,), jnp.int32), SMEM((n_pair * n_pair,), jnp.int32)],
        name="tables",
    )(jnp.stack([me_g, me_s]), pair_table.reshape(-1), counts, features)

    heads = w_value.reshape(width, HEADS, head_dim)
    blank = jnp.zeros((width, HEADS // 2, head_dim), BF16)
    w_val = jnp.concatenate(
        [heads[:, 0::2], blank, blank, heads[:, 1::2]], axis=-1
    ).reshape(width, 2 * width)
    w_val_t = jnp.concatenate([heads, jnp.zeros_like(heads)], axis=-1).reshape(width, 2 * width).T

    def pair_exchange(arrays, r):
        return [lax.ppermute(a, "pair", [(i, i ^ r) for i in range(n_pair)]) for a in arrays]

    order = sorted(range(1, n_sub), key=lambda r: min(r, n_sub - r))

    def run(hosts, sends, tab, features, w_val, w_val_t):
        got = {r: [None] * CHUNKS for r in range(n_pair)}
        for c in range(CHUNKS):
            got[0][c] = sends[c]
            for r in sorted(range(1, n_pair), reverse=True):
                got[r][c] = pair_exchange([sends[r * CHUNKS + c]], r)[0]
        held = [None] * (n_sub * CHUNKS)
        for c in range(CHUNKS):
            packed = pl.pallas_call(
                functools.partial(zpack_kernel, lay),
                in_specs=[smem] + [vmem] * n_pair,
                out_specs=[vmem] * n_sub,
                out_shape=[shaped(2, rows, width)] * n_sub,
                name="sub_pack",
            )(tab, *[got[r][c] for r in range(n_pair)])
            held[c] = packed[0]
            for r in order:
                held[r * CHUNKS + c] = lax.ppermute(
                    packed[r], "sub", [((t + r) % n_sub, t) for t in hosts]
                )
        points = n_sub * kp_block
        messages = pl.pallas_call(
            functools.partial(attention_kernel, lay, head_dim),
            in_specs=[smem] + [vmem] * (3 + n_sub * CHUNKS),
            out_specs=[vmem] * n_sub,
            out_shape=[shaped(2, kp_block, width)] * n_sub,
            scratch_shapes=[
                VMEM((2, points, width), BF16),
                VMEM((2, points, width), BF16),
                VMEM((points, 2 * width), BF16),
                VMEM((2 * width, points), BF16),
                VMEM((2, points, points), BF16),
                SMEM((1,), jnp.int32),
            ],
            name="attention",
        )(tab, w_qk, w_val, w_val_t, *held)
        returned = [messages[0]]
        for r in range(1, n_sub):
            returned.append(
                lax.ppermute(messages[r], "sub", [(t, (t + r) % n_sub) for t in hosts])
            )
        homeward = pl.pallas_call(
            functools.partial(xpack_kernel, lay),
            in_specs=[smem] + [vmem] * n_sub,
            out_specs=[vmem] * n_pair,
            out_shape=[shaped(per_src, kp_block, width)] * n_pair,
            name="pair_pack",
        )(tab, *returned)
        home = [homeward[0]] + [
            pair_exchange([homeward[r]], r)[0] for r in range(1, n_pair)
        ]
        first = pl.pallas_call(
            functools.partial(update_kernel, lay, False),
            in_specs=[smem] + [vmem] * 4,
            out_specs=vmem,
            out_shape=shaped(img_grp, kp_block, width),
            scratch_shapes=[VMEM((kp_block, width), F32)],
            name="update_idle",
        )(tab, features, w_out, w_merge_in, w_merge_out)
        return pl.pallas_call(
            functools.partial(update_kernel_last, lay),
            in_specs=[smem] + [vmem] * (5 + n_pair),
            out_specs=vmem,
            out_shape=shaped(img_grp, kp_block, width),
            scratch_shapes=[VMEM((kp_block, width), F32)],
            name="update_used",
        )(tab, features, w_out, w_merge_in, w_merge_out, first, *home)

    args = (sends, tab, features, w_val, w_val_t)
    if lay.few_hosts == lay.all_hosts:
        return run(lay.all_hosts, *args)
    return lax.cond(
        compact[0] == 1,
        functools.partial(run, lay.few_hosts),
        functools.partial(run, lay.all_hosts),
        *args,
    )


def update_kernel_last(lay, tab, feats, w_out, w_in, w_up, first, *refs):
    out = refs[-2]

    def keep(i, c):
        n = tab[lay.idle + i]
        out[n] = first[n]
        return c

    lax.fori_loop(0, tab[lay.n_idle], keep, 0)
    update_kernel(lay, True, tab, feats, w_out, w_in, w_up, *refs)


def solution(mesh):
    in_specs = (
        P(("parts", "pair"), "sub", None),
        P("parts"),
        P("parts", None, None),
        P(),
        P(),
        P(),
        P(),
        P(),
    )
    out_specs = P(("parts", "pair"), "sub", None)
    return jax.shard_map(local, mesh=mesh, in_specs=in_specs, out_specs=out_specs, check_vma=False)
```

```python
import functools

import jax
import jax.numpy as jnp
from jax import lax
from jax.experimental import pallas as pl
from jax.experimental.pallas import tpu as pltpu
from jax.sharding import PartitionSpec as P

HEADS = 4
CHUNKS = 2
LN_EPS = 1e-05
SUM_LOW = 1e-25
SUM_HIGH = 1e25
MIB = 1024 * 1024


F32 = jnp.float32
BF16 = jnp.bfloat16
I32 = jnp.int32
SMEM = pltpu.SMEM
VMEM = pltpu.VMEM


def dot(a, b, dims=(((1,), (0,)), ((), ()))):
    return lax.dot_general(a, b, dims, preferred_element_type=F32)


def div(a, n):
    return a >> (n.bit_length() - 1) if n & (n - 1) == 0 else a // n


def mod(a, n):
    return a & (n - 1) if n & (n - 1) == 0 else a % n


def each(n, body):
    if n <= 256:
        for i in range(n):
            body(i)
    else:
        lax.fori_loop(0, n, lambda i, c: (body(i), c)[1], 0)


class Layout:
    def __init__(self, n_pair, n_sub, img_grp):
        self.n_pair, self.n_sub, self.img_grp = n_pair, n_sub, img_grp
        self.few = self.per_src = min(2 * n_sub // n_pair, n_sub)
        self.low = (n_sub - self.few) // 2
        self.hosts = tuple(range(self.low, self.low + self.few))
        self.cap = n_pair * self.few
        self.rounds = -(-n_pair * n_sub // self.cap)
        self.n_msg = n_pair * self.per_src
        at = 0
        for name, size in (
            ("send", self.n_msg),
            ("zsel", 2 * n_sub),
            ("xret", self.n_msg),
            ("live", 1),
            ("count", 2),
        ):
            setattr(self, name, at)
            at += size
        self.stride = at
        at *= self.rounds
        for name, size in (
            ("n_rounds", 1),
            ("n_used", 1),
            ("n_idle", 1),
            ("used", img_grp),
            ("idle", img_grp),
            ("uses", img_grp),
            ("me_sub", 1),
            ("mine", img_grp * self.n_msg),
        ):
            setattr(self, name, at)
            at += size
        self.size = at


def copy_sends(lay, base, tab, feats, outs, sem):
    rows = feats.shape[1] // CHUNKS
    copies = []
    for c in range(CHUNKS):
        for r in range(lay.n_pair):
            for k in range(lay.per_src):
                image = tab[base + lay.send + r * lay.per_src + k]
                copies.append(
                    pltpu.make_async_copy(
                        feats.at[image, pl.ds(c * rows, rows)],
                        outs[r * CHUNKS + c].at[k],
                        sem.at[len(copies)],
                    )
                )
    for copy in copies:
        copy.start()
    for copy in copies:
        copy.wait()


def table_kernel(lay, table, counts, feats, *refs):
    n_pair, n_sub, per_src = lay.n_pair, lay.n_sub, lay.per_src
    outs, (tab, spare), (used_up, sem) = refs[:-4], refs[-4:-2], refs[-2:]
    me_g, me_s = lax.axis_index("pair"), lax.axis_index("sub")

    def clear(i):
        tab[i] = 0

    def wipe(i):
        used_up[i] = 0

    each(lay.size - lay.img_grp * lay.n_msg, clear)
    each(lay.rounds * n_pair * n_pair, wipe)

    def slot(at, rank):
        owner, pos = div(at, n_sub), mod(at, n_sub)
        live = table[owner, pos, 0] >= 0

        @pl.when(live)
        def _():
            turn = div(rank, lay.cap)
            place = mod(rank, lay.cap)
            g = mod(place, n_pair)
            t = lay.low + div(place, n_pair)
            base = turn * lay.stride
            for side in range(2):
                image = table[owner, pos, side]
                p = div(image, lay.img_grp)
                count_at = (turn * n_pair + p) * n_pair + g
                k = used_up[count_at]
                used_up[count_at] = k + 1

                @pl.when(p == me_g)
                def _():
                    entry = (g ^ me_g) * per_src + k
                    own = image - p * lay.img_grp
                    tab[base + lay.send + entry] = own
                    n = tab[lay.uses + own]
                    tab[lay.mine + own * lay.n_msg + n] = turn * lay.n_msg + entry
                    tab[lay.uses + own] = n + 1

                @pl.when(g == me_g)
                def _():
                    entry = (p ^ me_g) * per_src + k
                    tab[base + lay.zsel + 2 * t + side] = entry
                    tab[base + lay.xret + entry] = 2 * mod(me_s - t + n_sub, n_sub) + side

                    @pl.when(t == me_s)
                    def _():
                        tab[base + lay.live] = 1
                        tab[base + lay.count + side] = counts[image]

        return rank + live.astype(I32)

    total = lax.fori_loop(0, n_pair * n_sub, slot, jnp.int32(0))
    tab[lay.n_rounds] = jnp.maximum((total + lay.cap - 1) // lay.cap, 1)
    tab[lay.me_sub] = me_s

    def sort(n, c):
        named = tab[lay.uses + n] > 0

        @pl.when(named)
        def _():
            at = tab[lay.n_used]
            tab[lay.used + at] = n
            tab[lay.n_used] = at + 1

        @pl.when(jnp.logical_not(named))
        def _():
            at = tab[lay.n_idle]
            tab[lay.idle + at] = n
            tab[lay.n_idle] = at + 1

        return c

    lax.fori_loop(0, lay.img_grp, sort, 0)
    copy_sends(lay, 0, tab, feats, outs, sem)


def resend_kernel(lay, turn, tab, feats, *refs):
    copy_sends(lay, turn[0] * lay.stride, tab, feats, refs[:-1], refs[-1])


def pick(refs, entry, width, put):
    which, at = div(entry, width), mod(entry, width)
    for r, ref in enumerate(refs):

        @pl.when(which == r)
        def _(ref=ref):
            put(ref[at])


def zpack_kernel(lay, turn, tab, *refs):
    n_sub = lay.n_sub
    base = turn[0] * lay.stride
    arrived, outs = refs[: lay.n_pair], refs[lay.n_pair :]
    for r in range(n_sub):
        t = mod(tab[lay.me_sub] - r + n_sub, n_sub)
        for side in range(2):

            def put(block, r=r, side=side):
                outs[r][side] = block

            pick(arrived, tab[base + lay.zsel + 2 * t + side], lay.per_src, put)


def xpack_kernel(lay, turn, tab, *refs):
    base = turn[0] * lay.stride
    returned, outs = refs[: lay.n_sub], refs[lay.n_sub :]
    for r in range(lay.n_pair):
        for k in range(lay.per_src):

            def put(block, r=r, k=k):
                outs[r][k] = block

            pick(returned, tab[base + lay.xret + r * lay.per_src + k], 2, put)


def attention_kernel(lay, head_dim, turn, tab, w_qk, w_val, *refs):
    n_sub = lay.n_sub
    n_in = n_sub * CHUNKS
    xs, outs = refs[:n_in], refs[n_in:-6]
    x, qk, val, val_t, exps, flag = refs[-6:]
    base = turn[0] * lay.stride
    chunk = xs[0].shape[1]
    kp_block = chunk * CHUNKS
    points = n_sub * kp_block
    width = 2 * head_dim
    scale = head_dim ** (-0.5)
    parts = 4
    part = points // parts
    ones = val_t.shape[1] - head_dim

    @pl.when(tab[base + lay.live] == 1)
    def _():
        for r in range(n_sub):
            for c in range(CHUNKS):
                at = r * kp_block + c * chunk
                for side in range(2):
                    x[side, at : at + chunk] = xs[r * CHUNKS + c][side]

        def valid(shape, axis, side):
            ids = lax.broadcasted_iota(I32, shape, axis)
            block = div(ids, kp_block)
            pos = mod(tab[lay.me_sub] + block, n_sub) * kp_block + (ids - block * kp_block)
            return pos < tab[base + lay.count + side]

        lane = lax.broadcasted_iota(I32, (1, width), 1) // head_dim

        def values(side):
            v = dot(x[side], w_val[...])
            ok = valid((points, 1), 0, side)
            for j in range(2):
                val[j] = jnp.where(ok, jnp.where(lane == j, v, 1.0), 0.0).astype(BF16)

        for side in range(2):
            qk[side] = dot(x[side], w_qk[...]).astype(BF16)
        values(1)
        ok_t = valid((1, points), 1, 0)
        vt = dot(x[0], w_val[...]).T
        vt = jnp.where(ok_t, vt, 0.0).astype(BF16)
        tail = jnp.broadcast_to(jnp.where(ok_t, 1.0, 0.0), (ones, points)).astype(BF16)
        for j in range(2):
            val_t[j, :head_dim] = vt[j * head_dim : (j + 1) * head_dim]
            val_t[j, head_dim:] = tail

        def write(side, row, msg):
            for i in range(msg.shape[0] // kp_block):
                outs[row // kp_block + i][side] = msg[i * kp_block : (i + 1) * kp_block].astype(BF16)

        def merge(sums):
            top = jnp.where(lane == 0, sums[0], sums[1])
            total = pltpu.roll(jnp.where(lane == 0, sums[1], sums[0]), head_dim, 1)
            return top / total, total

        low, high = [], []

        def seen(total):
            low.append(jnp.min(total, keepdims=True))
            high.append(jnp.max(total, keepdims=True))

        columns = []
        sums = [[], []]
        for j in range(2):
            for i in range(parts):
                q = qk[0, i * part : (i + 1) * part]
                q = jnp.where(lane == j, q * scale, 0.0).astype(BF16)
                e = jnp.exp(dot(q, qk[1], (((1,), (1,)), ((), ())))).astype(BF16)
                exps[j, i * part : (i + 1) * part] = e
                sums[j].append(dot(e, val[j]))
            out = dot(val_t[j], exps[j])
            total = out[head_dim : head_dim + 1]
            seen(total)
            columns.append(out[:head_dim] / total)
        for i in range(parts):
            msg, total = merge([sums[0][i], sums[1][i]])
            seen(total)
            write(0, i * part, msg)
        write(1, 0, jnp.concatenate(columns, axis=0).T)
        smallest = functools.reduce(jnp.minimum, low)
        largest = functools.reduce(jnp.maximum, high)
        sound = (smallest > SUM_LOW) & (largest < SUM_HIGH)
        flag[0] = jnp.max(jnp.where(sound, 1, 0))

        @pl.when(flag[0] == 0)
        def _():
            for side in range(2):
                values(1 - side)
                key_ok = valid((1, points), 1, 1 - side)
                for i in range(n_sub):
                    sums = []
                    for j in range(2):
                        q = qk[side, i * kp_block : (i + 1) * kp_block]
                        q = jnp.where(lane == j, q * scale, 0.0).astype(BF16)
                        s = dot(q, qk[1 - side], (((1,), (1,)), ((), ())))
                        s = jnp.where(key_ok, s, -jnp.inf)
                        e = jnp.exp(s - jnp.max(s, axis=1, keepdims=True)).astype(BF16)
                        sums.append(dot(e, val[j]))
                    write(side, i * kp_block, merge(sums)[0])


def update_image(own, mean, w_out, w_in, w_up):
    width = own.shape[1]
    hidden = dot(own, w_in[:width])
    if mean is not None:
        lifted = dot(mean, w_out[...]).astype(BF16)
        hidden = hidden + dot(lifted, w_in[width:])
    centered = hidden - jnp.mean(hidden, axis=-1, keepdims=True)
    variance = jnp.mean(centered * centered, axis=-1, keepdims=True)
    normed = centered * lax.rsqrt(variance + LN_EPS)
    active = 0.5 * normed * (1.0 + lax.erf(normed * (0.5**0.5)))
    return (own.astype(F32) + dot(active.astype(BF16), w_up[...])).astype(BF16)


def store_loop(count, image_of, compute, out, held, sem):
    def copy(i):
        slot = mod(i, 4)
        return pltpu.make_async_copy(held.at[slot], out.at[image_of(i)], sem.at[slot])

    rows = held.shape[1]

    def step(j, c):
        i = 2 * j
        new = compute([image_of(i), image_of(jnp.minimum(i + 1, count - 1))])
        for side in range(2):

            @pl.when(i + side >= 4)
            def _(side=side):
                copy(i + side - 4).wait()

            @pl.when(i + side < count)
            def _(side=side):
                held[mod(i + side, 4)] = new[side * rows : (side + 1) * rows]
                copy(i + side).start()

        return c

    lax.fori_loop(0, (count + 1) >> 1, step, 0)
    spilled = count & 1
    for back in range(1, 5):

        @pl.when((count >= back) & (back <= 4 - spilled))
        def _(back=back):
            copy(count - back).wait()


def idle_kernel(lay, tab, feats, w_in, w_up, out, held, sem):
    def compute(images):
        own = jnp.concatenate([feats[n] for n in images], axis=0)
        return update_image(own, None, None, w_in, w_up)

    store_loop(tab[lay.n_idle], lambda i: tab[lay.idle + i], compute, out, held, sem)


def used_kernel(lay, tab, feats, w_out, w_in, w_up, first, later, *refs):
    del first
    msgs, (out, held, total, late, sem, late_sem) = refs[:-6], refs[-6:]
    n_pair, per_src, n_msg = lay.n_pair, lay.per_src, lay.n_msg
    cols = late.shape[1]

    def mean_of(n, total):
        uses = tab[lay.uses + n]
        total[...] = jnp.zeros_like(total)

        def add(k, c):
            entry = tab[lay.mine + n * n_msg + k]

            @pl.when(entry < n_msg)
            def _():
                for p in range(2):

                    def put(block, p=p):
                        total[:, p * cols : (p + 1) * cols] += block.astype(F32)

                    pick(msgs[p * n_pair : (p + 1) * n_pair], entry, per_src, put)

            @pl.when(entry >= n_msg)
            def _():
                for p in range(2):
                    copy = pltpu.make_async_copy(later.at[p, entry - n_msg], late, late_sem)
                    copy.start()
                    copy.wait()
                    total[:, p * cols : (p + 1) * cols] += late[...].astype(F32)

            return c

        lax.fori_loop(0, uses, add, 0)
        return (total[...] / uses.astype(F32)).astype(BF16)

    def compute(images):
        own = jnp.concatenate([feats[n] for n in images], axis=0)
        mean = jnp.concatenate([mean_of(n, total.at[j]) for j, n in enumerate(images)], axis=0)
        return update_image(own, mean, w_out, w_in, w_up)

    store_loop(tab[lay.n_used], lambda i: tab[lay.used + i], compute, out, held, sem)


def local(features, counts, pair_table, w_qk, w_value, w_out, w_merge_in, w_merge_out):
    n_pair = lax.axis_size("pair")
    n_sub = lax.axis_size("sub")
    img_grp, kp_block, width = features.shape
    head_dim = width // HEADS
    cols = width // 2
    lay = Layout(n_pair, n_sub, img_grp)
    per_src = lay.per_src
    rows = kp_block // CHUNKS
    points = n_sub * kp_block
    smem = pl.BlockSpec(memory_space=SMEM)
    vmem = pl.BlockSpec(memory_space=VMEM)
    anyw = pl.BlockSpec(memory_space=pl.ANY)

    def shaped(*dims, dtype=BF16):
        return jax.ShapeDtypeStruct(dims, dtype)

    def grant(mib):
        return pltpu.CompilerParams(vmem_limit_bytes=mib * MIB)

    send_specs = [vmem] * (n_pair * CHUNKS)
    send_shapes = [shaped(per_src, rows, width)] * (n_pair * CHUNKS)
    send_sem = pltpu.SemaphoreType.DMA((n_pair * CHUNKS * per_src,))
    n_late = max(lay.rounds - 1, 1)
    *sends, tab, spare = pl.pallas_call(
        functools.partial(table_kernel, lay),
        in_specs=[smem, smem, anyw],
        out_specs=send_specs + [smem, anyw],
        out_shape=send_shapes
        + [
            shaped(lay.size, dtype=I32),
            shaped(2, n_late * lay.n_msg, kp_block, cols),
        ],
        scratch_shapes=[SMEM((lay.rounds * n_pair * n_pair,), I32), send_sem],
        compiler_params=grant(8),
        name="tables",
    )(pair_table, counts, features)

    def pair_exchange(a, r):
        return lax.ppermute(a, "pair", [(i, i ^ r) for i in range(n_pair)])

    near = sorted(range(1, n_sub), key=lambda r: min(r, n_sub - r))
    far = near[::-1]
    w_halves = [(w_qk[:, p * cols : (p + 1) * cols], w_value[:, p * cols : (p + 1) * cols]) for p in range(2)]

    def arrive(turn, tab, sends):
        got = [[None] * n_pair for _ in range(CHUNKS)]
        for c in range(CHUNKS):
            got[c][0] = sends[c]
            for r in range(n_pair - 1, 0, -1):
                got[c][r] = pair_exchange(sends[r * CHUNKS + c], r)
        held = [None] * (n_sub * CHUNKS)
        for c in range(CHUNKS):
            packed = pl.pallas_call(
                functools.partial(zpack_kernel, lay),
                in_specs=[smem, smem] + [vmem] * n_pair,
                out_specs=[vmem] * n_sub,
                out_shape=[shaped(2, rows, width)] * n_sub,
                compiler_params=grant(8),
                name="sub_pack",
            )(turn, tab, *got[c])
            held[c] = packed[0]
            for r in near:
                held[r * CHUNKS + c] = lax.ppermute(
                    packed[r], "sub", [((t + r) % n_sub, t) for t in lay.hosts]
                )
        return held, packed

    def answer(turn, tab, held):
        home = []
        for p in range(2):
            messages = pl.pallas_call(
                functools.partial(attention_kernel, lay, head_dim),
                in_specs=[smem, smem] + [vmem] * (2 + n_sub * CHUNKS),
                out_specs=[vmem] * n_sub,
                out_shape=[shaped(2, kp_block, cols)] * n_sub,
                scratch_shapes=[
                    VMEM((2, points, width), BF16),
                    VMEM((2, points, cols), BF16),
                    VMEM((2, points, cols), BF16),
                    VMEM((2, head_dim + 16, points), BF16),
                    VMEM((2, points, points), BF16),
                    SMEM((1,), I32),
                ],
                compiler_params=grant(32),
                name="attention",
            )(turn, tab, *w_halves[p], *held)
            returned = [messages[0]] + [None] * (n_sub - 1)
            for r in far:
                returned[r] = lax.ppermute(
                    messages[r], "sub", [(t, (t + r) % n_sub) for t in lay.hosts]
                )
            homeward = pl.pallas_call(
                functools.partial(xpack_kernel, lay),
                in_specs=[smem, smem] + [vmem] * n_sub,
                out_specs=[vmem] * n_pair,
                out_shape=[shaped(per_src, kp_block, cols)] * n_pair,
                compiler_params=grant(8),
                name="pair_pack",
            )(turn, tab, *returned)
            arrived = [homeward[0]] + [None] * (n_pair - 1)
            for r in range(n_pair - 1, 0, -1):
                arrived[r] = pair_exchange(homeward[r], r)
            home += arrived
        return home

    zero = jnp.zeros((1,), I32)
    held, packed = arrive(zero, tab, sends)
    tab_mid, _ = lax.optimization_barrier((tab, packed[0]))

    if lay.rounds > 1:

        def extra(q, buf):
            turn = jnp.full((1,), q, I32)
            again = pl.pallas_call(
                functools.partial(resend_kernel, lay),
                in_specs=[smem, smem, anyw],
                out_specs=send_specs,
                out_shape=send_shapes,
                scratch_shapes=[send_sem],
                compiler_params=grant(8),
                name="resend",
            )(turn, tab, features)
            more = answer(turn, tab, arrive(turn, tab, again)[0])
            block = jnp.stack(
                [jnp.concatenate(more[p * n_pair : (p + 1) * n_pair], axis=0) for p in range(2)]
            )
            return lax.dynamic_update_slice_in_dim(buf, block, (q - 1) * lay.n_msg, 1)

        spare = lax.fori_loop(1, tab_mid[lay.n_rounds], extra, spare)

    first = pl.pallas_call(
        functools.partial(idle_kernel, lay),
        in_specs=[smem] + [vmem] * 3,
        out_specs=anyw,
        out_shape=shaped(img_grp, kp_block, width),
        scratch_shapes=[VMEM((4, kp_block, width), BF16), pltpu.SemaphoreType.DMA((4,))],
        compiler_params=grant(16),
        name="update_idle",
    )(tab_mid, features, w_merge_in, w_merge_out)
    tab_late, first, spare = lax.optimization_barrier((tab, first, spare))
    home = answer(zero, tab_late, held)
    return pl.pallas_call(
        functools.partial(used_kernel, lay),
        in_specs=[smem] + [vmem] * 4 + [anyw, anyw] + [vmem] * len(home),
        out_specs=anyw,
        out_shape=shaped(img_grp, kp_block, width),
        scratch_shapes=[
            VMEM((4, kp_block, width), BF16),
            VMEM((2, kp_block, width), F32),
            VMEM((kp_block, cols), BF16),
            pltpu.SemaphoreType.DMA((4,)),
            pltpu.SemaphoreType.DMA,
        ],
        input_output_aliases={5: 0},
        compiler_params=grant(16),
        name="update_used",
    )(tab, features, w_out, w_merge_in, w_merge_out, first, spare, *home)


def solution(mesh):
    in_specs = (
        P(("parts", "pair"), "sub", None),
        P("parts"),
        P("parts", None, None),
        P(),
        P(),
        P(),
        P(),
        P(),
    )
    out_specs = P(("parts", "pair"), "sub", None)
    return jax.shard_map(local, mesh=mesh, in_specs=in_specs, out_specs=out_specs, check_vma=False)
```
